32 devices in a mesh: dp: 4 (over y, x), vocab: 8 (over z, core).
Axes of the slice: x: 2, y: 2, z: 4, core: 2. Of those that a mesh axis runs over, the one named last changes fastest.
Arguments:
- hidden: bfloat16 [512, 8192], P('dp', 'vocab'), may hold values from -20 to 20
- weight: bfloat16 [8192, 4752], P('dp', 'vocab'), may hold values from -0.198873782 to 0.198873782
- targets: int32 [512], P('dp'), may hold values from 0 to 4751
- loss_mask: int32 [512], P('dp'), may hold values 0 or 1
Outputs:
- grad_hidden: bfloat16 [512, 8192], P('dp', 'vocab')
- grad_weight: bfloat16 [8192, 4752], P('dp', 'vocab')
- token_loss: float32 [512], P('dp')
- grad_norm: float32 [], replicated
The draws below stay inside these ranges and needn't reach their ends.
All inputs are finite; a program needn't handle non-finite values. No bound on the sum of `loss_mask` on one device may be relied on, other than what follows from the above.
Results may differ from the reference program's by a relative error of at most 0.0034.
Values may be sent and summed in bfloat16 or wider, within the bound.
A program may use at most 128 MiB of HBM per device.

```python
import math
import jax
import jax.numpy as jnp
import numpy as np
from jax import lax

D = 8192
V_DEV = 594
VOCAB = 4752
TOKENS = 512
N_VOCAB = 8


def weight_column(key, column):
    column_key = jax.random.fold_in(jax.random.fold_in(key, 71), column)
    values = jnp.clip(jax.random.normal(column_key, (D,), jnp.float32), -6.0, 6.0)
    return values * (3.0 / math.sqrt(D))


def draw_weight(key, part):
    columns = jax.vmap(lambda column: weight_column(key, column))(jnp.arange(VOCAB, dtype=jnp.int32))
    return columns.T.astype(jnp.bfloat16)


def draw_hidden(key, part):
    drawn = jnp.clip(jax.random.normal(jax.random.fold_in(key, 13), (TOKENS, D), jnp.float32), -6.0, 6.0)
    return drawn.astype(jnp.bfloat16)


def set_ends(array, own_key, least, largest):
    longest = array.shape.index(max(array.shape))
    spots = []
    for shift in (0, 1):
        where = [jax.random.randint(jax.random.fold_in(own_key, axis), (), 0, length) for axis, length in enumerate(array.shape)]
        where[longest] = (where[longest] + shift) % array.shape[longest]
        spots.append(tuple(where))
    return array.at[spots[0]].set(least).at[spots[1]].set(largest)


def rank_table(number_of, lean):
    weights = [(1 << 20) // math.isqrt(rank ** lean) + 1 for rank in range(1, number_of + 1)]
    deviation = 1 + sum(weights) // (1 << 30)
    return np.cumsum(np.array([max(1, weight // deviation) for weight in weights]))


def ranked_ids(stream_key, shape, number_of, lean):
    listing = rank_table(number_of, lean)
    lot = jax.random.randint(jax.random.fold_in(stream_key, 1), shape, 0, int(listing[number_of - 1]))
    rank = jnp.searchsorted(jnp.asarray(listing, jnp.int32), lot, side="right")
    return jax.random.permutation(jax.random.fold_in(stream_key, 2), number_of)[rank].astype(jnp.int32)


def setup_inputs(seed: int = 0) -> dict:
    key_of = jax.random.split(jax.random.key(seed), 5)
    hidden = draw_hidden(jax.random.fold_in(key_of[4], 71), 0)
    weight = draw_weight(jax.random.fold_in(key_of[4], 71), 0)
    targets = set_ends(ranked_ids(key_of[2], (TOKENS,), VOCAB, 2), jax.random.fold_in(key_of[2], 3), 0, VOCAB - 1).astype(jnp.int32)
    loss_mask = set_ends((jax.random.randint(key_of[3], (TOKENS,), 0, 4) < 3).astype(jnp.int32), jax.random.fold_in(key_of[3], 1), 0, 1)
    return dict(hidden=hidden, weight=weight, targets=targets, loss_mask=loss_mask)


loss_scale = 16.0

def reference(hidden, weight, targets, loss_mask):
    logits = jnp.dot(hidden, weight, preferred_element_type=jnp.float32)
    row_top = lax.optimization_barrier(jnp.max(logits, axis=1, keepdims=True))
    log_total = row_top[:, 0] + jnp.log(lax.optimization_barrier(jnp.sum(jnp.exp(logits - row_top), axis=1)))
    onehot = (lax.broadcasted_iota(jnp.int32, logits.shape, 1) == targets[:, None]).astype(jnp.float32)
    target_logit = lax.optimization_barrier(jnp.sum(logits * onehot, axis=1))
    row_keep = loss_mask.astype(jnp.float32)
    token_loss = row_keep * (log_total - target_logit)
    softmax = jnp.exp(logits - log_total[:, None])
    dlogits = (loss_scale * row_keep[:, None] * (softmax - onehot)).astype(jnp.bfloat16)
    hidden_grad_full = lax.dot_general(dlogits, weight, (((1,), (1,)), ((), ())), preferred_element_type=jnp.float32)

    def weight_block(block_index):
        block_start = (block_index * V_DEV).astype(jnp.int32)
        grad_slice = lax.dynamic_slice_in_dim(dlogits, block_start, V_DEV, 1)
        grad_piece = lax.dot_general(hidden, grad_slice, (((0,), (0,)), ((), ())), preferred_element_type=jnp.float32)
        return (grad_piece.astype(jnp.bfloat16), jnp.sum(grad_piece * grad_piece))
    blocks, squares = lax.map(weight_block, jnp.arange(N_VOCAB, dtype=jnp.int32))
    grad_weight = jnp.transpose(blocks, (1, 0, 2)).reshape(D, V_DEV * N_VOCAB)
    grad_norm = jnp.sqrt(jnp.sum(squares) + jnp.sum(hidden_grad_full * hidden_grad_full))
    return (hidden_grad_full.astype(jnp.bfloat16), grad_weight, token_loss, grad_norm)
```

```python
import functools

import jax
import jax.numpy as jnp
from jax import lax
from jax.experimental import pallas as pl
from jax.experimental.pallas import tpu as pltpu
from jax.sharding import PartitionSpec as P

loss_scale = 16.0
MESH = pl.DeviceIdType.MESH
f32 = jnp.float32
bf16 = jnp.bfloat16
vmem_bytes = 67043328


def dot_nn(a, b):
    return jnp.dot(a, b, preferred_element_type=f32)


def dot_nt(a, b):
    return lax.dot_general(a, b, (((1,), (1,)), ((), ())), preferred_element_type=f32)


def each(count, body):
    if count <= 32:
        for s in range(count):
            body(s)
    else:

        def step(s, carry):
            body(s)
            return carry

        lax.fori_loop(0, count, step, 0)


def kernel(
    n, nv, cpc, nc,
    hid_in, w_in, tgt_in, keep_in,
    hg_out, wg_out, loss_out, norm_out,
    hid, tgt, keep, w, gat, hb, lp, lr, lg, tcol, kcol, st, sr, dall, ps, pr, gs, g1, g2, via, mid, n1,
    io, h1_s, h1_r, h2_s, h2_r, h3_s, h3_r, l_s, l_r, s_s, s_r, d_s, d_r,
    p_s, p_r, g1_s, g1_r, g2_s, g2_r, g3_r, via_r, n_s, n_r,
):
    T, F = hid.shape
    V = w.shape[0]
    Tc = T // nc
    bpd = nv // n
    zpd = bpd // cpc
    nz = nv // cpc
    k = lax.axis_index("dp")
    j = lax.axis_index("vocab")
    z, c = j // cpc, j % cpc

    def push(src, dst, ss, rs, dp, vocab):
        pltpu.make_async_remote_copy(
            src_ref=src, dst_ref=dst, send_sem=ss, recv_sem=rs,
            device_id={"dp": dp, "vocab": vocab}, device_id_type=MESH,
        ).start()

    def arrived(dst, sem):
        pltpu.make_async_copy(dst, dst, sem).wait()

    def turn(s, base, size):
        return lax.rem(base + s, size)

    def columns(q, core):
        if F % 128 == 0:
            return w[:, pl.ds(pl.multiple_of((q * cpc + core) * F, F), F)]
        out = w[:, q * cpc * F:(q * cpc + 1) * F]
        for a in range(1, cpc):
            out = jnp.where(core == a, w[:, (q * cpc + a) * F:(q * cpc + a + 1) * F], out)
        return out

    def to_wide(row):
        return jnp.transpose(jnp.broadcast_to(row, (128, T)))

    reads = [
        pltpu.make_async_copy(src, dst, io.at[a])
        for a, (src, dst) in enumerate(((hid_in, hid), (tgt_in, tgt), (keep_in, keep), (w_in, w)))
    ]
    for read in reads:
        read.start()

    barrier = pltpu.get_barrier_semaphore()

    def greet_vocab(s):
        pl.semaphore_signal(barrier, inc=1, device_id={"dp": k, "vocab": turn(s + 1, j, nv)}, device_id_type=MESH)

    def greet_dp(s):
        pl.semaphore_signal(barrier, inc=1, device_id={"dp": turn(s + 1, k, n), "vocab": j}, device_id_type=MESH)

    each(nv - 1, greet_vocab)
    each(n - 1, greet_dp)
    for read in reads[:3]:
        read.wait()
    pl.semaphore_wait(barrier, nv + n - 2)

    line = nz == 4
    half = z // 2

    def flip(b):
        return b + half * (3 - 2 * b)

    lead = flip(z)

    def gather(h):
        piece = hid.at[pl.ds(h * Tc, Tc)]
        gat[z, h] = hid[h * Tc:(h + 1) * Tc, :]

        def send(to):
            push(piece, gat.at[z, h], h1_s, h1_r.at[z, h], k, to * cpc + c)

        if line:
            send(flip(3 - lead))
            send(flip(2 - 2 * lead))

            @pl.when(lead == 0)
            def _():
                send(flip(1))
        else:
            each(nz - 1, lambda s: send(turn(s + 1, z, nz)))

    for h in range(min(nc, 2)):
        gather(h)
    if line:

        @pl.when(lead == 0)
        def _():
            g2[flip(3)] = jnp.zeros((nc, Tc, F), bf16)

    tcol[...] = to_wide(tgt[...].astype(f32)).astype(jnp.int32) - j * V
    kcol[...] = to_wide(keep[...].astype(f32)) * loss_scale

    def exchange(h):
        def one(b):
            i, bl = b // zpd, (b % zpd) * cpc + c
            src, dst = gat.at[b, h], hb.at[bl, h, k]

            @pl.when(i != k)
            def _():
                push(src, dst, h2_s, h2_r.at[h], i, j)

            @pl.when(i == k)
            def _():
                hb[bl, h, k] = gat[b, h]

        if line:
            one(z)
            b = flip(1 + lead)
            arrived(gat.at[b, h], h1_r.at[b, h])

            @pl.when(lead == 1)
            def _():
                push(gat.at[b, h], gat.at[b, h], h1_s, h1_r.at[b, h], k, flip(0) * cpc + c)

            one(b)
            for b in (flip(3 - 3 * lead), flip(2 + lead)):
                arrived(gat.at[b, h], h1_r.at[b, h])
                one(b)
        else:
            one(z)

            def rest(s):
                b = turn(s + 1, z, nz)
                arrived(gat.at[b, h], h1_r.at[b, h])
                one(b)

            each(nz - 1, rest)
        if h + 2 < nc:
            gather(h + 2)

    def swap(h):
        if n > 1:
            arrived(hb.at[pl.ds(0, zpd), h, pl.ds(0, n - 1)], h2_r.at[h])
        for d in range(1, cpc):
            for q in range(zpd):
                slot = hb.at[q * cpc + c, h]
                push(slot, slot, h3_s, h3_r.at[h], k, z * cpc + turn(d, c, cpc))

    def partial(h):
        total = None
        for q in range(zpd):
            term = dot_nt(hb[q * cpc + c, h].reshape(n * Tc, F), columns(q, c))
            total = term if total is None else total + term
        if cpc > 1:
            arrived(hb.at[pl.ds(0, (cpc - 1) * zpd), h], h3_r.at[h])
        for d in range(1, cpc):
            for q in range(zpd):
                other = turn(d, c, cpc)
                total += dot_nt(hb[q * cpc + other, h].reshape(n * Tc, F), columns(q, other))
        lp[h] = total.reshape(n, Tc, V)
        for s in range(1, n):
            t = turn(s, k, n)
            push(lp.at[h, t], lr.at[h, s - 1], l_s, l_r.at[h], t, j)

    def hot(h):
        return lax.broadcasted_iota(jnp.int32, (Tc, V), 1) == tcol[h * Tc:(h + 1) * Tc, :1]

    def statistics(h):
        own = lp[h, k]
        if n > 1:
            arrived(lr.at[h], l_r.at[h])
        for s in range(n - 1):
            own += lr[h, s]
        lg[h] = own
        top = jnp.max(own, axis=1, keepdims=True)
        part = jnp.sum(jnp.exp(own - top), axis=1, keepdims=True)
        hit = jnp.sum(jnp.where(hot(h), own, 0.0), axis=1, keepdims=True)
        lane = lax.broadcasted_iota(jnp.int32, (Tc, 128), 1)
        packed = [jnp.where(lane == 0, top, jnp.where(lane == 1, part, hit))]
        if h:
            packed.insert(0, jnp.zeros((h * Tc, 128), f32))
        if h + 1 < nc:
            packed.append(jnp.zeros(((nc - 1 - h) * Tc, 128), f32))
        mine = jnp.transpose(jnp.concatenate(packed, axis=0))[:8, :]
        st[h] = mine
        sr[h, j] = mine

        def tell(s):
            push(st.at[h], sr.at[h, j], s_s, s_r.at[h], k, turn(s + 1, j, nv))

        each(nv - 1, tell)

    def logit_grads(h):
        arrived(sr.at[h, pl.ds(0, nv - 1)], s_r.at[h])
        stats = sr[h]
        tops, parts, hits = stats[:, 0, :], stats[:, 1, :], stats[:, 2, :]
        row_top = jnp.max(tops, axis=0, keepdims=True)
        exp_sum = jnp.sum(parts * jnp.exp(tops - row_top), axis=0, keepdims=True)
        target_logit = jnp.sum(hits, axis=0, keepdims=True)
        log_total = row_top + jnp.log(exp_sum)
        loss = keep[...].astype(f32) * (log_total - target_logit)
        if h:
            lane = lax.broadcasted_iota(jnp.int32, (1, T), 1)
            loss = jnp.where(lane >= h * Tc, loss, loss_out[...])
        loss_out[...] = loss
        soft = jnp.exp(lg[h] - to_wide(log_total)[h * Tc:(h + 1) * Tc, :1])
        scale = kcol[h * Tc:(h + 1) * Tc, :1]
        dall[h, k] = (scale * (soft - jnp.where(hot(h), 1.0, 0.0))).astype(bf16)
        src = dall.at[h, k]
        for s in range(1, n):
            push(src, src, d_s, d_r.at[h], turn(s, k, n), j)

    def other_part(h):
        if n > 1:
            arrived(dall.at[h, pl.ds(0, n - 1)], d_r.at[h])
        rows = dall[h].reshape(n * Tc, V)
        for d in range(1, cpc):
            other = turn(d, c, cpc)
            for q in range(zpd):
                ps[h, d - 1, q] = dot_nn(rows, columns(q, other))
            push(ps.at[h, d - 1], pr.at[h, d - 1], p_s, p_r.at[h], k, z * cpc + other)

    def relay(src, i, q, h):
        to = i * zpd + q
        dst = g2.at[z, h]
        far = flip(to) == 3 if line else False

        def forward():
            @pl.when(to == z)
            def _():
                g2[z, h] = src[...]

            @pl.when(to != z)
            def _():
                sem = g2_r.at[h]
                if not line:
                    push(src, dst, g2_s, sem, k, to * cpc + c)
                    return

                beyond = (lead == 0) & (flip(to) == 2)

                @pl.when(beyond)
                def _():
                    push(src, dst, g2_s, g3_r.at[h], k, to * cpc + c)

                @pl.when(jnp.logical_not(beyond))
                def _():
                    push(src, dst, g2_s, sem, k, to * cpc + c)

        if not line:
            forward()
            return
        pl.when(jnp.logical_not(far))(forward)

        @pl.when(far & (lead == 0))
        def _():
            push(src, via.at[h], g2_s, via_r.at[h], k, flip(1) * cpc + c)

        @pl.when(far & (lead == 1))
        def _():
            mid[h] = src[...]

    def combine(h):
        if not line:
            return

        @pl.when(lead == 1)
        def _():
            arrived(via.at[h], via_r.at[h])
            mid[h] = (mid[h].astype(f32) + via[h].astype(f32)).astype(bf16)
            push(mid.at[h], g2.at[z, h], g2_s, g2_r.at[h], k, flip(3) * cpc + c)

    def own_part(h):
        rows = dall[h].reshape(n * Tc, V)
        for q in range(zpd):
            part_sum = dot_nn(rows, columns(q, c))
            for d in range(1, cpc):
                if q == 0 and d == 1:
                    arrived(pr.at[h], p_r.at[h])
                part_sum += pr[h, d - 1, q]
            gs[h, :, q] = part_sum.astype(bf16).reshape(n, Tc, F)
        for s in range(1, n):
            t = turn(s, k, n)
            push(gs.at[h, t], g1.at[k, h], g1_s, g1_r.at[k, h], t, j)
        for q in range(zpd):
            relay(gs.at[h, k, q], k, q, h)

    def pass_on(h):
        for s in range(1, n):
            i = turn(s, k, n)
            arrived(g1.at[i, h], g1_r.at[i, h])
            for q in range(zpd):
                relay(g1.at[i, h, q], i, q, h)

    def collect(h):
        def take(src):
            return g2[src, h].astype(f32)

        if line:
            arrived(g2.at[pl.ds(0, 2), h], g2_r.at[h])

            @pl.when(lead == 1)
            def _():
                arrived(g2.at[0, h], g3_r.at[h])

            total = take(z) + take(flip(1 - lead)) + take(flip(2)) + take(flip(3))
        else:
            arrived(g2.at[pl.ds(0, nz - 1), h], g2_r.at[h])
            if nz <= 16:
                total = take(0)
                for src in range(1, nz):
                    total += take(src)
            else:
                total = lax.fori_loop(0, nz, lambda s, acc: acc + take(s), jnp.zeros((Tc, F), f32))
        hg_out[h * Tc:(h + 1) * Tc, :] = total.astype(bf16)
        return jnp.sum(total * total)

    def run(stage, h):
        return stage(h)

    for step in range(nc + 5):
        if step < nc:
            run(exchange, step)
        if 0 <= step - 4 < nc:
            run(other_part, step - 4)
        if 0 <= step - 1 < nc:
            run(swap, step - 1)
        if 0 <= step - 3 < nc:
            run(logit_grads, step - 3)
        if 0 <= step - 1 < nc:
            if step == 1:
                reads[3].wait()
            run(partial, step - 1)
        if 0 <= step - 4 < nc:
            run(own_part, step - 4)
        if 0 <= step - 2 < nc:
            run(statistics, step - 2)
        if 0 <= step - 5 < nc - 1:
            run(pass_on, step - 5)
            run(combine, step - 5)

    grads = jnp.transpose(dall[...].reshape(n * T, V))
    squares = jnp.zeros((1, F), f32)
    for bl in range(bpd):
        if bl == bpd // 2:
            run(pass_on, nc - 1)
            run(combine, nc - 1)
        grad = dot_nn(grads, hb[bl].reshape(n * T, F))
        wg_out[:, bl * F:(bl + 1) * F] = grad.astype(bf16)
        squares += jnp.sum(grad * grad, axis=0, keepdims=True)

    both = jnp.sum(squares)
    for h in range(nc):
        both += run(collect, h)

    peers = n * nv
    me = k * nv + j
    n1[me] = jnp.full((1, 128), both, f32)

    def tell_all(s):
        to = turn(s + 1, me, peers)
        push(n1.at[me], n1.at[me], n_s, n_r, to // nv, to % nv)

    each(peers - 1, tell_all)
    arrived(n1.at[pl.ds(0, peers - 1)], n_r)
    norm_out[...] = jnp.sqrt(jnp.sum(n1[...], axis=0))[:, :1]

    arrived(gat.at[pl.ds(0, nz - 1)], h1_s)
    arrived(g2.at[pl.ds(0, nz - 1)], g2_s)
    arrived(sr.at[:, pl.ds(0, nv - 1)], s_s)
    arrived(n1.at[pl.ds(0, peers - 1)], n_s)
    if n > 1:
        arrived(gat.at[pl.ds(0, nz - zpd)], h2_s)
        arrived(lr, l_s)
        arrived(dall.at[:, pl.ds(0, n - 1)], d_s)
        arrived(g1.at[pl.ds(0, n - 1)], g1_s)
    if cpc > 1:
        arrived(hb.at[pl.ds(0, (cpc - 1) * zpd)], h3_s)
        arrived(ps, p_s)


def pad(size, unit):
    return -(-size // unit) * unit


def store(*refs):
    sems = refs[-1]
    copies = [pltpu.make_async_copy(refs[a], refs[a + 4], sems.at[a]) for a in (1, 0, 2, 3)]
    for copy in copies:
        copy.start()
    for copy in copies:
        copy.wait()


def on_device(n, nv, hidden, weight, targets, loss_mask):
    T, F = hidden.shape
    R, V = weight.shape
    bpd = nv // n
    cpc = 2 if bpd % 2 == 0 else 1
    zpd, nz = bpd // cpc, nv // cpc
    nc = 4 if T % 64 == 0 else 1
    Tc = T // nc
    dma = pltpu.SemaphoreType.DMA
    vmem = pl.BlockSpec(memory_space=pltpu.VMEM)
    hbm = pl.BlockSpec(memory_space=pltpu.HBM)
    others = max(cpc - 1, 1)
    kept = 2 * (pad(V, 8) * pad(R, 128) + pad(T, 16) * pad(F, 128)) + 4 * (pad(T, 128) + 128)
    results = pl.pallas_call(
        functools.partial(kernel, n, nv, cpc, nc),
        out_shape=(
            pltpu.VMEM((T, F), bf16),
            pltpu.VMEM((V, R), bf16),
            pltpu.VMEM((1, T), f32),
            pltpu.VMEM((1, 1), f32),
        ),
        in_specs=[hbm] * 4,
        out_specs=(vmem, vmem, vmem, vmem),
        scratch_shapes=[
            pltpu.VMEM((T, F), bf16),
            pltpu.VMEM((1, T), jnp.int32),
            pltpu.VMEM((1, T), jnp.int32),
            pltpu.VMEM((V, R), bf16),
            pltpu.VMEM((nz, nc, Tc, F), bf16),
            pltpu.VMEM((bpd, nc, n, Tc, F), bf16),
            pltpu.VMEM((nc, n, Tc, V), f32),
            pltpu.VMEM((nc, n - 1, Tc, V), f32),
            pltpu.VMEM((nc, Tc, V), f32),
            pltpu.VMEM((T, 128), jnp.int32),
            pltpu.VMEM((T, 128), f32),
            pltpu.VMEM((nc, 8, T), f32),
            pltpu.VMEM((nc, nv, 8, T), f32),
            pltpu.VMEM((nc, n, Tc, V), bf16),
            pltpu.VMEM((nc, others, zpd, n * Tc, F), f32),
            pltpu.VMEM((nc, others, zpd, n * Tc, F), f32),
            pltpu.VMEM((nc, n, zpd, Tc, F), bf16),
            pltpu.VMEM((n, nc, zpd, Tc, F), bf16),
            pltpu.VMEM((nz, nc, Tc, F), bf16),
            pltpu.VMEM((nc, Tc, F), bf16),
            pltpu.VMEM((nc, Tc, F), bf16),
            pltpu.VMEM((n * nv, 1, 128), f32),
            dma((4,)), dma, dma((nz, nc)), dma, dma((nc,)), dma, dma((nc,)), dma, dma((nc,)), dma, dma((nc,)), dma, dma((nc,)),
            dma, dma((nc,)), dma, dma((n, nc)), dma, dma((nc,)), dma((nc,)), dma((nc,)), dma, dma,
        ],
        compiler_params=pltpu.CompilerParams(
            collective_id=0, has_side_effects=True, vmem_limit_bytes=vmem_bytes - kept - 8192
        ),
    )(hidden, weight.T, targets.reshape(1, T), loss_mask.reshape(1, T))
    hg, wg, loss, norm = pl.pallas_call(
        store,
        out_shape=tuple(jax.ShapeDtypeStruct(r.shape, r.dtype) for r in results),
        in_specs=[pl.BlockSpec(memory_space=pl.ANY)] * 4,
        out_specs=(hbm,) * 4,
        scratch_shapes=[dma((4,))],
        compiler_params=pltpu.CompilerParams(vmem_limit_bytes=1024 * 1024),
    )(*results)
    return hg, wg.T, loss.reshape(T), norm.reshape(())


def solution(mesh):
    placed = (P("dp", "vocab"), P("dp", "vocab"), P("dp"), P("dp"))
    return jax.shard_map(
        functools.partial(on_device, mesh.shape["dp"], mesh.shape["vocab"]),
        mesh=mesh,
        in_specs=placed,
        out_specs=(P("dp", "vocab"), P("dp", "vocab"), P("dp"), P()),
        check_vma=False,
    )
```

```python
import functools
import math

import jax
import jax.numpy as jnp
from jax import lax
from jax.experimental import pallas as pl
from jax.experimental.pallas import tpu as pltpu
from jax.sharding import PartitionSpec as P

loss_scale = 16.0
MESH = pl.DeviceIdType.MESH
f32 = jnp.float32
bf16 = jnp.bfloat16
vmem_bytes = 67043328


def dot_nn(a, b):
    return jnp.dot(a, b, preferred_element_type=f32)


def each(count, body):
    if count <= 32:
        for s in range(count):
            body(s)
    else:

        def step(s, carry):
            body(s)
            return carry

        lax.fori_loop(0, count, step, 0)


def kernel(
    n, nv, cpc, sizes,
    hid_in, w_in, tgt_in, keep_in,
    hg_out, wg_out, loss_out, norm_out,
    hid, tgt, keep, w, wt, gat, hb, lp, lr, lg, tcol, kcol, st, sr, dall, ps, pr, gs, g1, g2, via, mid, gt, n1,
    io, h1_s, h1_r, h2_s, h2_r, h3_s, h3_r, l_s, l_r, s_s, s_r, d_s, d_r,
    p_s, p_r, g1_s, g1_r, g2_s, g2_r, g3_r, via_r, n_s, n_r,
):
    T, F = hid.shape
    V = w.shape[0]
    nc = len(sizes)
    starts = [sum(sizes[:h]) for h in range(nc)]
    unit = math.gcd(*sizes)
    bpd = nv // n
    zpd = bpd // cpc
    nz = nv // cpc
    k = lax.axis_index("dp")
    j = lax.axis_index("vocab")
    z, c = j // cpc, j % cpc

    def push(src, dst, ss, rs, dp, vocab):
        pltpu.make_async_remote_copy(
            src_ref=src, dst_ref=dst, send_sem=ss, recv_sem=rs,
            device_id={"dp": dp, "vocab": vocab}, device_id_type=MESH,
        ).start()

    def arrived(dst, sem):
        pltpu.make_async_copy(dst, dst, sem).wait()

    def peer(s):
        return (n - 1 - k, k + 1 - 2 * (k % 2), turn(2, k, n))[s - 1] if n == 4 else turn(s, k, n)

    def mine(h):
        return pl.ds(starts[h], sizes[h])

    def every(h):
        return pl.ds(n * starts[h], n * sizes[h])

    def of(t, h):
        return pl.ds(pl.multiple_of(n * starts[h] + t * sizes[h], unit), sizes[h])

    def turn(s, base, size):
        return lax.rem(base + s, size)

    def columns(q, core):
        if F % 128 == 0:
            return w[:, pl.ds(pl.multiple_of((q * cpc + core) * F, F), F)]
        out = w[:, q * cpc * F:(q * cpc + 1) * F]
        for a in range(1, cpc):
            out = jnp.where(core == a, w[:, (q * cpc + a) * F:(q * cpc + a + 1) * F], out)
        return out

    def rows_of(q, core):
        return wt[pl.ds(pl.multiple_of((q * cpc + core) * F, F), F), :]

    def to_wide(row):
        return jnp.transpose(jnp.broadcast_to(row, (128, T)))

    reads = [
        pltpu.make_async_copy(src, dst, io.at[a])
        for a, (src, dst) in enumerate(((hid_in, hid), (tgt_in, tgt), (keep_in, keep), (w_in, w)))
    ]
    for read in reads:
        read.start()

    barrier = pltpu.get_barrier_semaphore()

    def greet_vocab(s):
        pl.semaphore_signal(barrier, inc=1, device_id={"dp": k, "vocab": turn(s + 1, j, nv)}, device_id_type=MESH)

    def greet_dp(s):
        pl.semaphore_signal(barrier, inc=1, device_id={"dp": turn(s + 1, k, n), "vocab": j}, device_id_type=MESH)

    each(nv - 1, greet_vocab)
    each(n - 1, greet_dp)
    for read in reads[:3]:
        read.wait()
    pl.semaphore_wait(barrier, nv + n - 2)

    line = nz == 4
    half = z // 2

    def flip(b):
        return b + half * (3 - 2 * b)

    lead = flip(z)

    def gather(h):
        piece = hid.at[mine(h)]
        gat[z, mine(h), :] = hid[mine(h), :]

        def send(to):
            push(piece, gat.at[z, mine(h)], h1_s, h1_r.at[z, h], k, to * cpc + c)

        if line:
            send(flip(3 - lead))
            send(flip(2 - 2 * lead))

            @pl.when(lead == 0)
            def _():
                send(flip(1))
        else:
            each(nz - 1, lambda s: send(turn(s + 1, z, nz)))

    for h in range(min(nc, 2)):
        gather(h)
    if line:

        @pl.when(lead == 0)
        def _():
            g2[flip(3)] = jnp.zeros((T, F), bf16)

    reads[3].wait()
    wt[...] = jnp.transpose(w[...])
    tcol[...] = to_wide(tgt[...].astype(f32)).astype(jnp.int32) - j * V
    kcol[...] = to_wide(keep[...].astype(f32)) * loss_scale

    def exchange(h):
        def one(b):
            i, bl = b // zpd, (b % zpd) * cpc + c
            src, dst = gat.at[b, mine(h)], hb.at[bl, of(k, h)]

            @pl.when(i != k)
            def _():
                push(src, dst, h2_s, h2_r.at[h], i, j)

            @pl.when(i == k)
            def _():
                hb[bl, of(k, h), :] = gat[b, mine(h), :]

        if line:
            one(z)
            b = flip(1 + lead)
            arrived(gat.at[b, mine(h)], h1_r.at[b, h])

            @pl.when(lead == 1)
            def _():
                push(gat.at[b, mine(h)], gat.at[b, mine(h)], h1_s, h1_r.at[b, h], k, flip(0) * cpc + c)

            one(b)
            for b in (flip(3 - 3 * lead), flip(2 + lead)):
                arrived(gat.at[b, mine(h)], h1_r.at[b, h])
                one(b)
        else:
            one(z)

            def rest(s):
                b = turn(s + 1, z, nz)
                arrived(gat.at[b, mine(h)], h1_r.at[b, h])
                one(b)

            each(nz - 1, rest)
        if h + 2 < nc:
            gather(h + 2)

    def swap(h):
        if n > 1:
            arrived(hb.at[pl.ds(0, zpd), pl.ds(0, (n - 1) * sizes[h])], h2_r.at[h])
        for d in range(1, cpc):
            for q in range(zpd):
                slot = hb.at[q * cpc + c, every(h)]
                push(slot, slot, h3_s, h3_r.at[h], k, z * cpc + turn(d, c, cpc))

    def theirs(s, h):
        return pl.ds((n - 1) * starts[h] + (s - 1) * sizes[h], sizes[h])

    def partial(h):
        total = None
        for q in range(zpd):
            term = dot_nn(hb[q * cpc + c, every(h), :], rows_of(q, c))
            total = term if total is None else total + term
        if cpc > 1:
            arrived(hb.at[pl.ds(0, (cpc - 1) * zpd), every(h)], h3_r.at[h])
        for d in range(1, cpc):
            for q in range(zpd):
                other = turn(d, c, cpc)
                total += dot_nn(hb[q * cpc + other, every(h), :], rows_of(q, other))
        lp[every(h), :] = total
        for s in range(1, n):
            t = peer(s)
            push(lp.at[of(t, h)], lr.at[theirs(s, h)], l_s, l_r.at[h], t, j)

    def hot(h):
        return lax.broadcasted_iota(jnp.int32, (sizes[h], V), 1) == tcol[mine(h), :][:, :1]

    def statistics(h):
        own = lp[of(k, h), :]
        if n > 1:
            arrived(lr.at[pl.ds(0, (n - 1) * sizes[h])], l_r.at[h])
        for s in range(1, n):
            own += lr[theirs(s, h), :]
        lg[mine(h), :] = own
        top = jnp.max(own, axis=1, keepdims=True)
        part = jnp.sum(jnp.exp(own - top), axis=1, keepdims=True)
        hit = jnp.sum(jnp.where(hot(h), own, 0.0), axis=1, keepdims=True)
        lane = lax.broadcasted_iota(jnp.int32, (sizes[h], 128), 1)
        packed = [jnp.where(lane == 0, top, jnp.where(lane == 1, part, hit))]
        if h:
            packed.insert(0, jnp.zeros((starts[h], 128), f32))
        if h + 1 < nc:
            packed.append(jnp.zeros((T - starts[h] - sizes[h], 128), f32))
        told = jnp.transpose(jnp.concatenate(packed, axis=0))[:8, :]
        st[h] = told
        sr[h, j] = told

        def tell(s):
            push(st.at[h], sr.at[h, j], s_s, s_r.at[h], k, turn(s + 1, j, nv))

        each(nv - 1, tell)

    def logit_grads(h):
        arrived(sr.at[h, pl.ds(0, nv - 1)], s_r.at[h])
        stats = sr[h]
        tops, parts, hits = stats[:, 0, :], stats[:, 1, :], stats[:, 2, :]
        row_top = jnp.max(tops, axis=0, keepdims=True)
        exp_sum = jnp.sum(parts * jnp.exp(tops - row_top), axis=0, keepdims=True)
        target_logit = jnp.sum(hits, axis=0, keepdims=True)
        log_total = row_top + jnp.log(exp_sum)
        loss = keep[...].astype(f32) * (log_total - target_logit)
        if h:
            lane = lax.broadcasted_iota(jnp.int32, (1, T), 1)
            loss = jnp.where(lane >= starts[h], loss, loss_out[...])
        loss_out[...] = loss
        soft = jnp.exp(lg[mine(h), :] - to_wide(log_total)[starts[h]:starts[h] + sizes[h], :1])
        scale = kcol[mine(h), :][:, :1]
        dall[of(k, h), :] = (scale * (soft - jnp.where(hot(h), 1.0, 0.0))).astype(bf16)
        src = dall.at[of(k, h)]
        for s in range(1, n):
            push(src, src, d_s, d_r.at[h], peer(s), j)

    def other_part(h):
        if n > 1:
            arrived(dall.at[pl.ds(0, (n - 1) * sizes[h])], d_r.at[h])
        rows = dall[every(h), :]
        for d in range(1, cpc):
            other = turn(d, c, cpc)
            for q in range(zpd):
                ps[d - 1, q, every(h), :] = dot_nn(rows, columns(q, other))
            push(ps.at[d - 1, :, every(h)], pr.at[d - 1, :, every(h)], p_s, p_r.at[h], k, z * cpc + other)

    def relay(src, i, q, h):
        to = i * zpd + q
        dst = g2.at[z, mine(h)]
        far = flip(to) == 3 if line else False

        def forward():
            @pl.when(to == z)
            def _():
                g2[z, mine(h), :] = src[...]

            @pl.when(to != z)
            def _():
                sem = g2_r.at[h]
                if not line:
                    push(src, dst, g2_s, sem, k, to * cpc + c)
                    return

                beyond = (lead == 0) & (flip(to) == 2)

                @pl.when(beyond)
                def _():
                    push(src, dst, g2_s, g3_r.at[h], k, to * cpc + c)

                @pl.when(jnp.logical_not(beyond))
                def _():
                    push(src, dst, g2_s, sem, k, to * cpc + c)

        if not line:
            forward()
            return
        pl.when(jnp.logical_not(far))(forward)

        @pl.when(far & (lead == 0))
        def _():
            push(src, via.at[mine(h)], g2_s, via_r.at[h], k, flip(1) * cpc + c)

        @pl.when(far & (lead == 1))
        def _():
            mid[mine(h), :] = src[...]

    def combine(h):
        if not line:
            return

        @pl.when(lead == 1)
        def _():
            arrived(via.at[mine(h)], via_r.at[h])
            mid[mine(h), :] = (mid[mine(h), :].astype(f32) + via[mine(h), :].astype(f32)).astype(bf16)
            push(mid.at[mine(h)], g2.at[z, mine(h)], g2_s, g2_r.at[h], k, flip(3) * cpc + c)

    def own_part(h):
        rows = dall[every(h), :]
        for q in range(zpd):
            part_sum = dot_nn(rows, columns(q, c))
            for d in range(1, cpc):
                if q == 0 and d == 1:
                    arrived(pr.at[:, :, every(h)], p_r.at[h])
                part_sum += pr[d - 1, q, every(h), :]
            gs[q, every(h), :] = part_sum.astype(bf16)
        for s in range(1, n):
            t = peer(s)
            push(gs.at[:, of(t, h)], g1.at[k, :, mine(h)], g1_s, g1_r.at[k, h], t, j)
        for q in range(zpd):
            relay(gs.at[q, of(k, h)], k, q, h)

    def pass_on(h):
        def one(i):
            arrived(g1.at[i, :, mine(h)], g1_r.at[i, h])
            for q in range(zpd):
                relay(g1.at[i, q, mine(h)], i, q, h)

        if line:
            for d in (3, 2, 1, 0):
                i = flip(d)
                pl.when(i != k)(functools.partial(one, i))
        else:
            for s in range(1, n):
                one(turn(s, k, n))

    def collect(h):
        def take(src):
            return g2[src, mine(h), :].astype(f32)

        if line:
            arrived(g2.at[pl.ds(0, 2), mine(h)], g2_r.at[h])

            @pl.when(lead == 1)
            def _():
                arrived(g2.at[0, mine(h)], g3_r.at[h])

            total = take(z) + take(flip(1 - lead)) + take(flip(2)) + take(flip(3))
        else:
            arrived(g2.at[pl.ds(0, nz - 1), mine(h)], g2_r.at[h])
            if nz <= 16:
                total = take(0)
                for src in range(1, nz):
                    total += take(src)
            else:
                total = lax.fori_loop(0, nz, lambda s, acc: acc + take(s), jnp.zeros((sizes[h], F), f32))
        hg_out[mine(h), :] = total.astype(bf16)
        sums.append(jnp.sum(total * total))

    def run(stage, h):
        return stage(h)

    def weight_grad(bl):
        if bl == 0:
            gt[...] = jnp.transpose(dall[...])
        grad = dot_nn(gt[...], hb[bl])
        wg_out[:, bl * F:(bl + 1) * F] = grad.astype(bf16)
        sums.append(jnp.sum(grad * grad))

    sums = []
    plan = [(at + gap * (4 * (starts[h] + sizes[h]) / T - 1), stage, h) for stage, at, gap in (
        (exchange, 8, 4), (swap, 12.5, 4), (partial, 13, 4), (statistics, 18.5, 4), (logit_grads, 22, 4), (other_part, 26, 4),
        (own_part, 28, 4), (pass_on, 33, 4), (combine, 38, 4), (collect, 60, 1),
    ) for h in range(nc)]
    plan += [(43 + 16 * bl / bpd, weight_grad, bl) for bl in range(bpd)]
    for _, stage, h in sorted(plan, key=lambda entry: entry[0]):
        run(stage, h)

    both = sum(sums)

    peers = n * nv
    me = k * nv + j
    n1[me] = jnp.full((1, 128), both, f32)

    def tell_all(s):
        to = turn(s + 1, me, peers)
        push(n1.at[me], n1.at[me], n_s, n_r, to // nv, to % nv)

    each(peers - 1, tell_all)
    arrived(n1.at[pl.ds(0, peers - 1)], n_r)
    norm_out[...] = jnp.sqrt(jnp.sum(n1[...], axis=0))[:, :1]

    arrived(gat.at[pl.ds(0, nz - 1)], h1_s)
    arrived(g2.at[pl.ds(0, nz - 1)], g2_s)
    arrived(sr.at[:, pl.ds(0, nv - 1)], s_s)
    arrived(n1.at[pl.ds(0, peers - 1)], n_s)
    if n > 1:
        arrived(gat.at[pl.ds(0, nz - zpd)], h2_s)
        arrived(lr, l_s)
        arrived(dall.at[pl.ds(0, (n - 1) * T)], d_s)
        arrived(g1.at[pl.ds(0, n - 1)], g1_s)
    if cpc > 1:
        arrived(hb.at[pl.ds(0, (cpc - 1) * zpd)], h3_s)
        arrived(ps, p_s)


def pad(size, unit):
    return -(-size // unit) * unit


def store(*refs):
    sems = refs[-1]
    copies = [pltpu.make_async_copy(refs[a], refs[a + 4], sems.at[a]) for a in (1, 0, 2, 3)]
    for copy in copies:
        copy.start()
    for copy in copies:
        copy.wait()


def on_device(n, nv, hidden, weight, targets, loss_mask):
    T, F = hidden.shape
    R, V = weight.shape
    bpd = nv // n
    cpc = 2 if bpd % 2 == 0 else 1
    zpd, nz = bpd // cpc, nv // cpc
    sizes = [T // 8 * part for part in (1, 1, 2, 2, 1, 1)] if T % 128 == 0 else [T]
    nc = len(sizes)
    dma = pltpu.SemaphoreType.DMA
    vmem = pl.BlockSpec(memory_space=pltpu.VMEM)
    hbm = pl.BlockSpec(memory_space=pltpu.HBM)
    others = max(cpc - 1, 1)
    kept = 2 * (pad(V, 8) * pad(R, 128) + pad(T, 16) * pad(F, 128)) + 4 * (pad(T, 128) + 128)
    results = pl.pallas_call(
        functools.partial(kernel, n, nv, cpc, sizes),
        out_shape=(
            pltpu.VMEM((T, F), bf16),
            pltpu.VMEM((V, R), bf16),
            pltpu.VMEM((1, T), f32),
            pltpu.VMEM((1, 1), f32),
        ),
        in_specs=[hbm] * 4,
        out_specs=(vmem, vmem, vmem, vmem),
        scratch_shapes=[
            pltpu.VMEM((T, F), bf16),
            pltpu.VMEM((1, T), jnp.int32),
            pltpu.VMEM((1, T), jnp.int32),
            pltpu.VMEM((V, R), bf16),
            pltpu.VMEM((R, V), bf16),
            pltpu.VMEM((nz, T, F), bf16),
            pltpu.VMEM((bpd, n * T, F), bf16),
            pltpu.VMEM((n * T, V), f32),
            pltpu.VMEM((max(n - 1, 1) * T, V), f32),
            pltpu.VMEM((T, V), f32),
            pltpu.VMEM((T, 128), jnp.int32),
            pltpu.VMEM((T, 128), f32),
            pltpu.VMEM((nc, 8, T), f32),
            pltpu.VMEM((nc, nv, 8, T), f32),
            pltpu.VMEM((n * T, V), bf16),
            pltpu.VMEM((others, zpd, n * T, F), f32),
            pltpu.VMEM((others, zpd, n * T, F), f32),
            pltpu.VMEM((zpd, n * T, F), bf16),
            pltpu.VMEM((n, zpd, T, F), bf16),
            pltpu.VMEM((nz, T, F), bf16),
            pltpu.VMEM((T, F), bf16),
            pltpu.VMEM((T, F), bf16),
            pltpu.VMEM((V, n * T), bf16),
            pltpu.VMEM((n * nv, 1, 128), f32),
            dma((4,)), dma, dma((nz, nc)), dma, dma((nc,)), dma, dma((nc,)), dma, dma((nc,)), dma, dma((nc,)), dma, dma((nc,)),
            dma, dma((nc,)), dma, dma((n, nc)), dma, dma((nc,)), dma((nc,)), dma((nc,)), dma, dma,
        ],
        compiler_params=pltpu.CompilerParams(
            collective_id=0, has_side_effects=True, vmem_limit_bytes=vmem_bytes - kept - 8192
        ),
    )(hidden, weight.T, targets.reshape(1, T), loss_mask.reshape(1, T))
    hg, wg, loss, norm = pl.pallas_call(
        store,
        out_shape=tuple(jax.ShapeDtypeStruct(r.shape, r.dtype) for r in results),
        in_specs=[pl.BlockSpec(memory_space=pl.ANY)] * 4,
        out_specs=(hbm,) * 4,
        scratch_shapes=[dma((4,))],
        compiler_params=pltpu.CompilerParams(vmem_limit_bytes=1024 * 1024),
    )(*results)
    return hg, wg.T, loss.reshape(T), norm.reshape(())


def solution(mesh):
    placed = (P("dp", "vocab"), P("dp", "vocab"), P("dp"), P("dp"))
    return jax.shard_map(
        functools.partial(on_device, mesh.shape["dp"], mesh.shape["vocab"]),
        mesh=mesh,
        in_specs=placed,
        out_specs=(P("dp", "vocab"), P("dp", "vocab"), P("dp"), P()),
        check_vma=False,
    )
```

```python
import functools
import math

import jax
import jax.numpy as jnp
from jax import lax
from jax.experimental import pallas as pl
from jax.experimental.pallas import tpu as pltpu
from jax.sharding import PartitionSpec as P

loss_scale = 16.0
MESH = pl.DeviceIdType.MESH
f32 = jnp.float32
bf16 = jnp.bfloat16
vmem_bytes = 67043328


def dot_nn(a, b):
    return jnp.dot(a, b, preferred_element_type=f32)


def each(count, body):
    if count <= 32:
        for s in range(count):
            body(s)
    else:

        def step(s, carry):
            body(s)
            return carry

        lax.fori_loop(0, count, step, 0)


def kernel(
    n, nv, cpc, sizes,
    hid_in, w_in, tgt_in, keep_in,
    hg_out, wg_out, loss_out, norm_out,
    hid, tgt, keep, w, wt, gat, hb, lp, lr, lg, tcol, kcol, st, sr, dall, ps, pr, gs, g1, g2, via, mid, gt, lx, x_r, n1,
    io, h1_s, h1_r, h2_s, h2_r, h3_s, h3_r, l_s, l_r, s_s, s_r, d_s, d_r,
    p_s, p_r, g1_s, g1_r, g2_s, g2_r, g3_r, via_r, n_s, n_r,
):
    T, F = hid.shape
    V = w.shape[0]
    nc = len(sizes)
    starts = [sum(sizes[:h]) for h in range(nc)]
    unit = math.gcd(*sizes)
    bpd = nv // n
    zpd = bpd // cpc
    nz = nv // cpc
    k = lax.axis_index("dp")
    j = lax.axis_index("vocab")
    z, c = j // cpc, j % cpc

    def push(src, dst, ss, rs, dp, vocab):
        pltpu.make_async_remote_copy(
            src_ref=src, dst_ref=dst, send_sem=ss, recv_sem=rs,
            device_id={"dp": dp, "vocab": vocab}, device_id_type=MESH,
        ).start()

    def arrived(dst, sem):
        pltpu.make_async_copy(dst, dst, sem).wait()

    def peer(s):
        return (n - 1 - k, k + 1 - 2 * (k % 2), turn(2, k, n))[s - 1] if n == 4 else turn(s, k, n)

    square = n == 4 and unit % 16 == 0

    def part_of(t, h, a):
        size = sizes[h] // 2
        return pl.ds(pl.multiple_of(n * starts[h] + t * sizes[h] + a * size, unit // 2), size)

    def mine(h):
        return pl.ds(starts[h], sizes[h])

    def every(h):
        return pl.ds(n * starts[h], n * sizes[h])

    def of(t, h):
        return pl.ds(pl.multiple_of(n * starts[h] + t * sizes[h], unit), sizes[h])

    def turn(s, base, size):
        return lax.rem(base + s, size)

    def columns(q, core):
        if F % 128 == 0:
            return w[:, pl.ds(pl.multiple_of((q * cpc + core) * F, F), F)]
        out = w[:, q * cpc * F:(q * cpc + 1) * F]
        for a in range(1, cpc):
            out = jnp.where(core == a, w[:, (q * cpc + a) * F:(q * cpc + a + 1) * F], out)
        return out

    def rows_of(q, core):
        return wt[pl.ds(pl.multiple_of((q * cpc + core) * F, F), F), :]

    def to_wide(row):
        return jnp.transpose(jnp.broadcast_to(row, (128, T)))

    reads = [
        pltpu.make_async_copy(src, dst, io.at[a])
        for a, (src, dst) in enumerate(((hid_in, hid), (tgt_in, tgt), (keep_in, keep), (w_in, w)))
    ]
    for read in reads:
        read.start()

    barrier = pltpu.get_barrier_semaphore()

    def greet_vocab(s):
        pl.semaphore_signal(barrier, inc=1, device_id={"dp": k, "vocab": turn(s + 1, j, nv)}, device_id_type=MESH)

    def greet_dp(s):
        pl.semaphore_signal(barrier, inc=1, device_id={"dp": turn(s + 1, k, n), "vocab": j}, device_id_type=MESH)

    each(nv - 1, greet_vocab)
    each(n - 1, greet_dp)
    for read in reads[:3]:
        read.wait()
    pl.semaphore_wait(barrier, nv + n - 2)

    line = nz == 4
    half = z // 2

    def flip(b):
        return b + half * (3 - 2 * b)

    lead = flip(z)

    def gather(h):
        piece = hid.at[mine(h)]
        gat[z, mine(h), :] = hid[mine(h), :]

        def send(to):
            push(piece, gat.at[z, mine(h)], h1_s, h1_r.at[z, h], k, to * cpc + c)

        if line:
            send(flip(3 - lead))
            send(flip(2 - 2 * lead))

            @pl.when(lead == 0)
            def _():
                send(flip(1))
        else:
            each(nz - 1, lambda s: send(turn(s + 1, z, nz)))

    for h in range(min(nc, 2)):
        gather(h)
    if line:

        @pl.when(lead == 0)
        def _():
            g2[flip(3)] = jnp.zeros((T, F), bf16)

    reads[3].wait()
    wt[...] = jnp.transpose(w[...])
    tcol[...] = to_wide(tgt[...].astype(f32)).astype(jnp.int32) - j * V
    kcol[...] = to_wide(keep[...].astype(f32)) * loss_scale

    def exchange(h):
        def one(b):
            i, bl = b // zpd, (b % zpd) * cpc + c
            src, dst = gat.at[b, mine(h)], hb.at[bl, of(k, h)]

            @pl.when(i != k)
            def _():
                push(src, dst, h2_s, h2_r.at[h], i, j)

            @pl.when(i == k)
            def _():
                hb[bl, of(k, h), :] = gat[b, mine(h), :]

        if line:
            one(z)
            b = flip(1 + lead)
            arrived(gat.at[b, mine(h)], h1_r.at[b, h])

            @pl.when(lead == 1)
            def _():
                push(gat.at[b, mine(h)], gat.at[b, mine(h)], h1_s, h1_r.at[b, h], k, flip(0) * cpc + c)

            one(b)
            for b in (flip(3 - 3 * lead), flip(2 + lead)):
                arrived(gat.at[b, mine(h)], h1_r.at[b, h])
                one(b)
        else:
            one(z)

            def rest(s):
                b = turn(s + 1, z, nz)
                arrived(gat.at[b, mine(h)], h1_r.at[b, h])
                one(b)

            each(nz - 1, rest)
        if h + 2 < nc:
            gather(h + 2)

    def swap(h):
        if n > 1:
            arrived(hb.at[pl.ds(0, zpd), pl.ds(0, (n - 1) * sizes[h])], h2_r.at[h])
        for d in range(1, cpc):
            for q in range(zpd):
                slot = hb.at[q * cpc + c, every(h)]
                push(slot, slot, h3_s, h3_r.at[h], k, z * cpc + turn(d, c, cpc))

    def theirs(s, h):
        return pl.ds((n - 1) * starts[h] + (s - 1) * sizes[h], sizes[h])

    def partial(h):
        total = None
        for q in range(zpd):
            term = dot_nn(hb[q * cpc + c, every(h), :], rows_of(q, c))
            total = term if total is None else total + term
        if cpc > 1:
            arrived(hb.at[pl.ds(0, (cpc - 1) * zpd), every(h)], h3_r.at[h])
        for d in range(1, cpc):
            for q in range(zpd):
                other = turn(d, c, cpc)
                total += dot_nn(hb[q * cpc + other, every(h), :], rows_of(q, other))
        lp[every(h), :] = total
        if square:
            for a in (0, 1):
                size = sizes[h] // 2
                push(lp.at[part_of(peer(1), h, a)], lx.at[a, pl.ds(starts[h] // 2, size)], l_s, x_r.at[h], peer(2 + a), j)
            for a in (0, 1):
                push(lp.at[part_of(peer(2 + a), h, a)], lr.at[half_of(a, h, a)], l_s, l_r.at[h], peer(2 + a), j)
            return
        for s in range(1, n):
            t = peer(s)
            push(lp.at[of(t, h)], lr.at[theirs(s, h)], l_s, l_r.at[h], t, j)

    def half_of(s, h, a):
        size = sizes[h] // 2
        return pl.ds((n - 1) * starts[h] + s * sizes[h] + a * size, size)

    def across(h):
        if not square:
            return
        size = sizes[h] // 2
        arrived(lx.at[:, pl.ds(0, size)], x_r.at[h])
        for a in (0, 1):
            rows, t = part_of(peer(3 - a), h, a), peer(3 - a)
            lp[rows, :] = lp[rows, :] + lx[a, pl.ds(starts[h] // 2, size), :]
            push(lp.at[rows], lr.at[half_of(1 - a, h, a)], l_s, l_r.at[h], t, j)

    def hot(h):
        return lax.broadcasted_iota(jnp.int32, (sizes[h], V), 1) == tcol[mine(h), :][:, :1]

    def statistics(h):
        own = lp[of(k, h), :]
        if n > 1:
            arrived(lr.at[pl.ds(0, (2 if square else n - 1) * sizes[h])], l_r.at[h])
        for s in range(1, 3 if square else n):
            own += lr[theirs(s, h), :]
        lg[mine(h), :] = own
        top = jnp.max(own, axis=1, keepdims=True)
        part = jnp.sum(jnp.exp(own - top), axis=1, keepdims=True)
        hit = jnp.sum(jnp.where(hot(h), own, 0.0), axis=1, keepdims=True)
        lane = lax.broadcasted_iota(jnp.int32, (sizes[h], 128), 1)
        packed = [jnp.where(lane == 0, top, jnp.where(lane == 1, part, hit))]
        if h:
            packed.insert(0, jnp.zeros((starts[h], 128), f32))
        if h + 1 < nc:
            packed.append(jnp.zeros((T - starts[h] - sizes[h], 128), f32))
        told = jnp.transpose(jnp.concatenate(packed, axis=0))[:8, :]
        st[h] = told
        sr[h, j] = told

        def tell(s):
            push(st.at[h], sr.at[h, j], s_s, s_r.at[h], k, turn(s + 1, j, nv))

        each(nv - 1, tell)

    def logit_grads(h):
        arrived(sr.at[h, pl.ds(0, nv - 1)], s_r.at[h])
        stats = sr[h]
        tops, parts, hits = stats[:, 0, :], stats[:, 1, :], stats[:, 2, :]
        row_top = jnp.max(tops, axis=0, keepdims=True)
        exp_sum = jnp.sum(parts * jnp.exp(tops - row_top), axis=0, keepdims=True)
        target_logit = jnp.sum(hits, axis=0, keepdims=True)
        log_total = row_top + jnp.log(exp_sum)
        loss = keep[...].astype(f32) * (log_total - target_logit)
        if h:
            lane = lax.broadcasted_iota(jnp.int32, (1, T), 1)
            loss = jnp.where(lane >= starts[h], loss, loss_out[...])
        loss_out[...] = loss
        soft = jnp.exp(lg[mine(h), :] - to_wide(log_total)[starts[h]:starts[h] + sizes[h], :1])
        scale = kcol[mine(h), :][:, :1]
        dall[of(k, h), :] = (scale * (soft - jnp.where(hot(h), 1.0, 0.0))).astype(bf16)
        src = dall.at[of(k, h)]
        for s in range(1, n):
            push(src, src, d_s, d_r.at[h], peer(s), j)

    def other_part(h):
        if n > 1:
            arrived(dall.at[pl.ds(0, (n - 1) * sizes[h])], d_r.at[h])
        rows = dall[every(h), :]
        for d in range(1, cpc):
            other = turn(d, c, cpc)
            for q in range(zpd):
                ps[d - 1, q, every(h), :] = dot_nn(rows, columns(q, other))
            push(ps.at[d - 1, :, every(h)], pr.at[d - 1, :, every(h)], p_s, p_r.at[h], k, z * cpc + other)

    def relay(src, i, q, h):
        to = i * zpd + q
        dst = g2.at[z, mine(h)]
        far = flip(to) == 3 if line else False

        def forward():
            @pl.when(to == z)
            def _():
                g2[z, mine(h), :] = src[...]

            @pl.when(to != z)
            def _():
                sem = g2_r.at[h]
                if not line:
                    push(src, dst, g2_s, sem, k, to * cpc + c)
                    return

                beyond = (lead == 0) & (flip(to) == 2)

                @pl.when(beyond)
                def _():
                    push(src, dst, g2_s, g3_r.at[h], k, to * cpc + c)

                @pl.when(jnp.logical_not(beyond))
                def _():
                    push(src, dst, g2_s, sem, k, to * cpc + c)

        if not line:
            forward()
            return
        pl.when(jnp.logical_not(far))(forward)

        @pl.when(far & (lead == 0))
        def _():
            push(src, via.at[mine(h)], g2_s, via_r.at[h], k, flip(1) * cpc + c)

        @pl.when(far & (lead == 1))
        def _():
            mid[mine(h), :] = src[...]

    def combine(h):
        if not line:
            return

        @pl.when(lead == 1)
        def _():
            arrived(via.at[mine(h)], via_r.at[h])
            mid[mine(h), :] = (mid[mine(h), :].astype(f32) + via[mine(h), :].astype(f32)).astype(bf16)
            push(mid.at[mine(h)], g2.at[z, mine(h)], g2_s, g2_r.at[h], k, flip(3) * cpc + c)

    def own_part(h):
        rows = dall[every(h), :]
        for q in range(zpd):
            part_sum = dot_nn(rows, columns(q, c))
            for d in range(1, cpc):
                if q == 0 and d == 1:
                    arrived(pr.at[:, :, every(h)], p_r.at[h])
                part_sum += pr[d - 1, q, every(h), :]
            gs[q, every(h), :] = part_sum.astype(bf16)
        for s in range(1, n):
            t = peer(s)
            push(gs.at[:, of(t, h)], g1.at[k, :, mine(h)], g1_s, g1_r.at[k, h], t, j)
        for q in range(zpd):
            relay(gs.at[q, of(k, h)], k, q, h)

    def pass_on(h):
        def one(i):
            arrived(g1.at[i, :, mine(h)], g1_r.at[i, h])
            for q in range(zpd):
                relay(g1.at[i, q, mine(h)], i, q, h)

        if line:
            for d in (3, 2, 1, 0):
                i = flip(d)
                pl.when(i != k)(functools.partial(one, i))
        else:
            for s in range(1, n):
                one(turn(s, k, n))

    def collect(h):
        def take(src):
            return g2[src, mine(h), :].astype(f32)

        if line:
            arrived(g2.at[pl.ds(0, 2), mine(h)], g2_r.at[h])

            @pl.when(lead == 1)
            def _():
                arrived(g2.at[0, mine(h)], g3_r.at[h])

            total = take(z) + take(flip(1 - lead)) + take(flip(2)) + take(flip(3))
        else:
            arrived(g2.at[pl.ds(0, nz - 1), mine(h)], g2_r.at[h])
            if nz <= 16:
                total = take(0)
                for src in range(1, nz):
                    total += take(src)
            else:
                total = lax.fori_loop(0, nz, lambda s, acc: acc + take(s), jnp.zeros((sizes[h], F), f32))
        hg_out[mine(h), :] = total.astype(bf16)
        sums.append(jnp.sum(total * total))

    def run(stage, h):
        return stage(h)

    def weight_grad(bl):
        if bl == 0:
            gt[...] = jnp.transpose(dall[...])
        grad = dot_nn(gt[...], hb[bl])
        wg_out[:, bl * F:(bl + 1) * F] = grad.astype(bf16)
        sums.append(jnp.sum(grad * grad))

    sums = []
    plan = [(at + gap * (4 * (starts[h] + sizes[h]) / T - 1), stage, h) for stage, at, gap in (
        (exchange, 8, 4), (swap, 12.5, 4), (partial, 13, 4), (across, 16, 4), (statistics, 18.5, 4), (logit_grads, 22.0, 4), (other_part, 26.0, 4),
        (own_part, 28.0, 4), (pass_on, 33.0, 4), (combine, 38.0, 4), (collect, 44, 4),
    ) for h in range(nc)]
    plan += [(43 + 3 * bl / bpd, weight_grad, bl) for bl in range(bpd)]
    for _, stage, h in sorted(plan, key=lambda entry: entry[0]):
        run(stage, h)

    both = sum(sums)

    peers = n * nv
    me = k * nv + j
    n1[me] = jnp.full((1, 128), both, f32)

    def tell_all(s):
        to = turn(s + 1, me, peers)
        push(n1.at[me], n1.at[me], n_s, n_r, to // nv, to % nv)

    each(peers - 1, tell_all)
    arrived(n1.at[pl.ds(0, peers - 1)], n_r)
    norm_out[...] = jnp.sqrt(jnp.sum(n1[...], axis=0))[:, :1]

    arrived(gat.at[pl.ds(0, nz - 1)], h1_s)
    arrived(g2.at[pl.ds(0, nz - 1)], g2_s)
    arrived(sr.at[:, pl.ds(0, nv - 1)], s_s)
    arrived(n1.at[pl.ds(0, peers - 1)], n_s)
    if n > 1:
        arrived(gat.at[pl.ds(0, nz - zpd)], h2_s)
        arrived(lp.at[pl.ds(0, (n - 1) * T)], l_s)
        arrived(dall.at[pl.ds(0, (n - 1) * T)], d_s)
        arrived(g1.at[pl.ds(0, n - 1)], g1_s)
    if cpc > 1:
        arrived(hb.at[pl.ds(0, (cpc - 1) * zpd)], h3_s)
        arrived(ps, p_s)


def pad(size, unit):
    return -(-size // unit) * unit


def store(*refs):
    sems = refs[-1]
    copies = [pltpu.make_async_copy(refs[a], refs[a + 4], sems.at[a]) for a in (1, 0, 2, 3)]
    for copy in copies:
        copy.start()
    for copy in copies:
        copy.wait()


def on_device(n, nv, hidden, weight, targets, loss_mask):
    T, F = hidden.shape
    R, V = weight.shape
    bpd = nv // n
    cpc = 2 if bpd % 2 == 0 else 1
    zpd, nz = bpd // cpc, nv // cpc
    sizes = [T // 8 * part for part in (1, 1, 2, 2, 1, 1)] if T % 128 == 0 else [T]
    nc = len(sizes)
    dma = pltpu.SemaphoreType.DMA
    vmem = pl.BlockSpec(memory_space=pltpu.VMEM)
    hbm = pl.BlockSpec(memory_space=pltpu.HBM)
    others = max(cpc - 1, 1)
    kept = 2 * (pad(V, 8) * pad(R, 128) + pad(T, 16) * pad(F, 128)) + 4 * (pad(T, 128) + 128)
    results = pl.pallas_call(
        functools.partial(kernel, n, nv, cpc, sizes),
        out_shape=(
            pltpu.VMEM((T, F), bf16),
            pltpu.VMEM((V, R), bf16),
            pltpu.VMEM((1, T), f32),
            pltpu.VMEM((1, 1), f32),
        ),
        in_specs=[hbm] * 4,
        out_specs=(vmem, vmem, vmem, vmem),
        scratch_shapes=[
            pltpu.VMEM((T, F), bf16),
            pltpu.VMEM((1, T), jnp.int32),
            pltpu.VMEM((1, T), jnp.int32),
            pltpu.VMEM((V, R), bf16),
            pltpu.VMEM((R, V), bf16),
            pltpu.VMEM((nz, T, F), bf16),
            pltpu.VMEM((bpd, n * T, F), bf16),
            pltpu.VMEM((n * T, V), f32),
            pltpu.VMEM((max(n - 1, 1) * T, V), f32),
            pltpu.VMEM((T, V), f32),
            pltpu.VMEM((T, 128), jnp.int32),
            pltpu.VMEM((T, 128), f32),
            pltpu.VMEM((nc, 8, T), f32),
            pltpu.VMEM((nc, nv, 8, T), f32),
            pltpu.VMEM((n * T, V), bf16),
            pltpu.VMEM((others, zpd, n * T, F), f32),
            pltpu.VMEM((others, zpd, n * T, F), f32),
            pltpu.VMEM((zpd, n * T, F), bf16),
            pltpu.VMEM((n, zpd, T, F), bf16),
            pltpu.VMEM((nz, T, F), bf16),
            pltpu.VMEM((T, F), bf16),
            pltpu.VMEM((T, F), bf16),
            pltpu.VMEM((V, n * T), bf16),
            pltpu.VMEM((2, max(T // 2, 8), V), f32),
            dma((nc,)),
            pltpu.VMEM((n * nv, 1, 128), f32),
            dma((4,)), dma, dma((nz, nc)), dma, dma((nc,)), dma, dma((nc,)), dma, dma((nc,)), dma, dma((nc,)), dma, dma((nc,)),
            dma, dma((nc,)), dma, dma((n, nc)), dma, dma((nc,)), dma((nc,)), dma((nc,)), dma, dma,
        ],
        compiler_params=pltpu.CompilerParams(
            collective_id=0, has_side_effects=True, vmem_limit_bytes=vmem_bytes - kept - 8192
        ),
    )(hidden, weight.T, targets.reshape(1, T), loss_mask.reshape(1, T))
    hg, wg, loss, norm = pl.pallas_call(
        store,
        out_shape=tuple(jax.ShapeDtypeStruct(r.shape, r.dtype) for r in results),
        in_specs=[pl.BlockSpec(memory_space=pl.ANY)] * 4,
        out_specs=(hbm,) * 4,
        scratch_shapes=[dma((4,))],
        compiler_params=pltpu.CompilerParams(vmem_limit_bytes=1024 * 1024),
    )(*results)
    return hg, wg.T, loss.reshape(T), norm.reshape(())


def solution(mesh):
    placed = (P("dp", "vocab"), P("dp", "vocab"), P("dp"), P("dp"))
    return jax.shard_map(
        functools.partial(on_device, mesh.shape["dp"], mesh.shape["vocab"]),
        mesh=mesh,
        in_specs=placed,
        out_specs=(P("dp", "vocab"), P("dp", "vocab"), P("dp"), P()),
        check_vma=False,
    )
```
